32 devices in a mesh: dp: 8 (over z, y), mp: 4 (over x, core).
Axes of the slice: x: 2, y: 2, z: 4, core: 2. Of those that a mesh axis runs over, the one named last changes fastest.
Arguments:
- queries: bfloat16 [256, 64, 128], P('dp', 'mp'), may hold values from -8 to 8
- lookup_sheets: bfloat16 [8192, 16, 8, 128], P('dp', None, 'mp'), may hold values from -6 to 6
- content_sheets: bfloat16 [8192, 16, 8, 128], P('dp', None, 'mp'), may hold values from -12 to 12
- page_table: int32 [256, 32], replicated, may hold values from 0 to 8191, as said below
- context_len: int32 [256], replicated, may hold values from 32 to 512, as said below
- out_weight: bfloat16 [8192, 8192], P('mp', 'dp'), may hold values from -0.0625 to 0.0625
Outputs:
- attention: bfloat16 [256, 64, 128], P('dp', 'mp')
- projected: bfloat16 [256, 8192], P('mp', 'dp')
The draws below stay inside these ranges and needn't reach their ends.
Inputs may be any that keep to these rules, and one draw needn't show every extreme that they name: `page_table`: every entry names a pool page, 0 to 8191, and every pool page appears exactly once in the whole table. `context_len`: each length lies between 32 and 512; most contexts are short, and some request has exactly 512 tokens.
All inputs are finite; a program needn't handle non-finite values.
Results may differ from the reference program's by a relative error of at most 0.0015.
Values may be sent and summed in bfloat16 or wider, within the bound.
A program may use at most 128 MiB of HBM per device.

```python
import jax
import jax.numpy as jnp
from jax import lax

D = 8192
ASKER_COUNT = 64
LOOKUP_COUNT = 8
SPAN_PER_ASKER = 128
SHEET_CAPACITY = 16
REQ = 256
SHEET_TOTAL = 8192
MAXPG = 32


def draw_context_len(key, part):
    key_len, key_pos = jax.random.split(jax.random.fold_in(key, 11))
    longest = MAXPG * SHEET_CAPACITY
    lowest = max(longest // 16, 1)
    drawn = jax.random.randint(key_len, (REQ,), 0, longest, dtype=jnp.int32)
    skewed = drawn * drawn // longest * drawn // longest
    lengths = lowest + skewed * (longest - lowest) // longest
    chosen = jax.random.randint(key_pos, (), 0, REQ, dtype=jnp.int32)
    return lengths.at[chosen].set(longest).astype(jnp.int32)


def draw_page_table(key, part):
    shuffled = jax.random.permutation(jax.random.fold_in(key, 23), REQ * MAXPG)
    return shuffled.reshape(REQ, MAXPG).astype(jnp.int32)


def levels(key, dims, cuts, least, top_value):
    def one(axis_at, shards_of):
        steps = jax.random.uniform(jax.random.fold_in(jax.random.fold_in(key, 6), axis_at), (shards_of,), jnp.float32, least / len(cuts), top_value / len(cuts))
        return jnp.repeat(jnp.exp(steps), dims[axis_at] // shards_of).reshape((-1,) + (1,) * (len(dims) - axis_at - 1))

    gain = one(*cuts[0])
    for cut in cuts[1:]:
        gain = gain * one(*cut)
    return gain


def bell_draw(rng, extent, width, reach, pieces=(), kind=jnp.bfloat16):
    loudness = levels(rng, extent, pieces, -0.22, 0.18) if pieces else 1.0
    values = jax.random.normal(rng, extent, jnp.float32) * width * loudness
    return jnp.minimum(jnp.maximum(values, -reach), reach).astype(kind)


def setup_inputs(seed: int = 0) -> dict:
    key_list = jax.random.split(jax.random.key(seed), 7)
    return {
        "queries": bell_draw(key_list[0], (REQ, ASKER_COUNT, SPAN_PER_ASKER), 1.5, 8.0, ((0, 8), (1, 4))),
        "lookup_sheets": bell_draw(key_list[1], (SHEET_TOTAL, SHEET_CAPACITY, LOOKUP_COUNT, SPAN_PER_ASKER), 1.0, 6.0, ((0, 8), (2, 4))),
        "content_sheets": bell_draw(key_list[2], (SHEET_TOTAL, SHEET_CAPACITY, LOOKUP_COUNT, SPAN_PER_ASKER), 2.0, 12.0, ((0, 8), (2, 4))),
        "page_table": draw_page_table(jax.random.fold_in(key_list[6], 71), 0),
        "context_len": draw_context_len(jax.random.fold_in(key_list[6], 71), 0),
        "out_weight": bell_draw(key_list[5], (ASKER_COUNT * SPAN_PER_ASKER, D), (ASKER_COUNT * SPAN_PER_ASKER) ** -0.5, 0.0625, ((0, 4), (1, 8))),
    }


def reference(queries, lookup_sheets, content_sheets, page_table, context_len, out_weight):
    cluster_member = ASKER_COUNT // LOOKUP_COUNT

    def one_request(inputs):
        asker_vector, page_ids, length = inputs
        keys = lookup_sheets[page_ids].astype(jnp.float32)
        values = content_sheets[page_ids].astype(jnp.float32)
        clustered_askers = asker_vector.reshape(LOOKUP_COUNT, cluster_member, SPAN_PER_ASKER).astype(jnp.float32)
        scores = jnp.einsum("kgd,ptkd->kgpt", clustered_askers, keys) * (SPAN_PER_ASKER ** -0.5)
        position = (jnp.arange(MAXPG, dtype=jnp.int32)[:, None] * SHEET_CAPACITY
                    + jnp.arange(SHEET_CAPACITY, dtype=jnp.int32)[None, :])
        is_valid = position < length
        scores = jnp.where(is_valid, scores, -1e30)
        page_peak = jnp.max(scores, axis=-1)
        weights = jnp.where(is_valid, jnp.exp(scores - page_peak[..., None]), 0.0)
        page_mass = jnp.sum(weights, axis=-1)
        rounded = lax.optimization_barrier(weights.astype(jnp.bfloat16)).astype(jnp.float32)
        page_acc = jnp.einsum("kgpt,ptkd->kgpd", rounded, values)
        peak_row = jnp.max(page_peak, axis=-1)
        factor = jnp.exp(page_peak - peak_row[..., None])
        acc_row = jnp.sum(page_acc * factor[..., None], axis=2)
        mass_row = jnp.sum(page_mass * factor, axis=2)
        return (acc_row / mass_row[..., None]).astype(jnp.bfloat16).reshape(ASKER_COUNT, SPAN_PER_ASKER)

    attention = lax.map(one_request, (queries, page_table, context_len))
    flat_rows = attention.reshape(attention.shape[0], ASKER_COUNT * SPAN_PER_ASKER)
    projected = jnp.dot(flat_rows, out_weight, preferred_element_type=jnp.float32).astype(jnp.bfloat16)
    return attention, projected
```

```python
import functools

import jax
import jax.numpy as jnp
from jax import lax
from jax.experimental import pallas as pl
from jax.experimental.pallas import tpu as pltpu
from jax.sharding import PartitionSpec as P

MESH = pl.DeviceIdType.MESH
NEG = -1e30
DEPTH = 4
PRE = 2


def axis_barrier(axes):
    barrier = pltpu.get_barrier_semaphore()
    total = 0
    for name in axes:
        n = lax.axis_size(name)
        me = lax.axis_index(name)
        for step in range(1, n):
            pl.semaphore_signal(
                barrier, inc=1, device_id={name: lax.rem(me + step, n)}, device_id_type=MESH
            )
        total += n - 1
    pl.semaphore_wait(barrier, total)


def gather_kernel(q_ref, all_ref, send_sem, recv_sem, own_sem):
    n = lax.axis_size("dp")
    me = lax.axis_index("dp")
    axis_barrier(("dp",))
    copies = []
    for step in range(1, n):
        copy = pltpu.make_async_remote_copy(
            src_ref=q_ref,
            dst_ref=all_ref.at[me],
            send_sem=send_sem.at[step],
            recv_sem=recv_sem.at[step],
            device_id={"dp": lax.rem(me + step, n)},
            device_id_type=MESH,
        )
        copy.start()
        copies.append(copy)
    own = pltpu.make_async_copy(q_ref, all_ref.at[me], own_sem)
    own.start()
    own.wait()
    for copy in copies:
        copy.wait()


def gather_queries(queries):
    n = lax.axis_size("dp")
    return pl.pallas_call(
        gather_kernel,
        out_shape=jax.ShapeDtypeStruct((n,) + queries.shape, queries.dtype),
        in_specs=[pl.BlockSpec(memory_space=pltpu.VMEM)],
        out_specs=pl.BlockSpec(memory_space=pltpu.VMEM),
        scratch_shapes=[
            pltpu.SemaphoreType.DMA((n,)),
            pltpu.SemaphoreType.DMA((n,)),
            pltpu.SemaphoreType.DMA,
        ],
        compiler_params=pltpu.CompilerParams(collective_id=0, has_side_effects=True),
    )(queries)


def attend_kernel(
    sizes, codes, counts, totals, q_ref, k_hbm, v_hbm, acc_ref, stat_ref,
    kbuf, vbuf, kmore, vmore, ksem, vsem, moresem,
):
    rows, max_pages, span, kv_local, blocks, code_base, unroll = sizes
    q_local, head_dim = q_ref.shape[1:]
    per = 128 // span
    held = per * PRE
    b = pl.program_id(0)
    f32 = jnp.float32

    def issue(block, slot):
        @pl.loop(0, rows)
        def _(r):
            row = block * rows + r

            @pl.loop(0, jnp.minimum(counts[row], held))
            def _(s):
                page = codes[row * max_pages + s] // code_base
                pltpu.make_async_copy(k_hbm.at[page], kbuf.at[slot, r * held + s], ksem.at[slot]).start()
                pltpu.make_async_copy(v_hbm.at[page], vbuf.at[slot, r * held + s], vsem.at[slot]).start()

    @pl.when(b == 0)
    def _():
        @pl.loop(0, DEPTH)
        def _(slot):
            @pl.loop(0, rows)
            def _(r):
                vbuf[slot, pl.ds(r * held, held)] = jnp.zeros((held, span, head_dim), vbuf.dtype)

        vmore[...] = jnp.zeros(vmore.shape, vmore.dtype)
        for first in range(min(DEPTH - 1, blocks)):
            issue(first, first)

    @pl.when(b + DEPTH - 1 < blocks)
    def _():
        issue(b + DEPTH - 1, lax.rem(b + DEPTH - 1, DEPTH))

    slot = lax.rem(b, DEPTH)
    total = totals[b]
    for bit in range((rows * held).bit_length()):
        size = 1 << bit
        if size > min(rows * held, k_hbm.shape[0]):
            break

        @pl.when((total >> bit) & 1 == 1)
        def _():
            pltpu.make_async_copy(k_hbm.at[pl.ds(0, size)], kbuf.at[slot, pl.ds(0, size)], ksem.at[slot]).wait()
            pltpu.make_async_copy(v_hbm.at[pl.ds(0, size)], vbuf.at[slot, pl.ds(0, size)], vsem.at[slot]).wait()

    lane = lax.broadcasted_iota(jnp.int32, (per * q_local, 128), 1)
    line = lax.broadcasted_iota(jnp.int32, (per * q_local, 128), 0)
    fits = (lane // span == line // q_local) & (
        lane % kv_local == (line % q_local) // (q_local // kv_local)
    )
    token = jnp.where(fits, (lane % span) // kv_local, code_base)
    stat_lane = lax.broadcasted_iota(jnp.int32, (q_local, 128), 1)
    scale = head_dim ** (-0.5)

    def chunk(r, first, keys, values):
        row = b * rows + r
        scores = lax.dot_general(
            q_ref[r], keys, (((1,), (1,)), ((), ())), preferred_element_type=f32
        ) * scale
        limits = [codes[row * max_pages + first + i] % code_base for i in range(per)]
        limit = jnp.concatenate([jnp.full((q_local, 128), x, jnp.int32) for x in limits], axis=0)
        valid = token < limit
        spread = jnp.where(valid, jnp.concatenate([scores] * per, axis=0), NEG)
        peak = jnp.max(spread, axis=1, keepdims=True)
        weights = jnp.where(valid, jnp.exp(spread - peak), 0.0)
        mass = jnp.sum(weights, axis=1, keepdims=True)
        acc = jnp.dot(weights.astype(jnp.bfloat16), values, preferred_element_type=f32)
        peak = peak.reshape(per, q_local, 1)
        top = jnp.max(peak, axis=0)
        factor = jnp.exp(peak - top[None])
        mass = jnp.sum(mass.reshape(per, q_local, 1) * factor, axis=0)
        acc = jnp.sum(acc.reshape(per, q_local, head_dim) * factor, axis=0)
        return top, mass, acc

    def put_stats(r, stats, top, mass):
        return jnp.where(stat_lane == r, top, stats[0]), jnp.where(stat_lane == r, mass, stats[1])

    def first_chunk(r, stats):
        at = pl.ds(r * held, per)
        top, mass, acc = chunk(
            r, 0, kbuf[slot, at].reshape(128, head_dim), vbuf[slot, at].reshape(128, head_dim)
        )
        acc_ref[r] = acc
        return put_stats(r, stats, top, mass)

    def body(i, stats):
        for u in range(unroll):
            stats = first_chunk(i * unroll + u, stats)
        return stats

    empty = (jnp.full((q_local, 128), NEG, f32), jnp.zeros((q_local, 128), f32))
    stats = lax.fori_loop(0, rows // unroll, body, empty)
    stat_ref[0], stat_ref[1] = stats

    def merge(r, part):
        top, mass, acc = part
        here = stat_lane == r
        old_top = jnp.max(jnp.where(here, stat_ref[0], NEG), axis=1, keepdims=True)
        old_mass = jnp.sum(jnp.where(here, stat_ref[1], 0.0), axis=1, keepdims=True)
        new_top = jnp.maximum(old_top, top)
        old_f = jnp.exp(old_top - new_top)
        new_f = jnp.exp(top - new_top)
        acc_ref[r] = acc_ref[r] * old_f + acc * new_f
        stat_ref[0] = jnp.where(here, new_top, stat_ref[0])
        stat_ref[1] = jnp.where(here, old_mass * old_f + mass * new_f, stat_ref[1])

    @pl.loop(0, rows)
    def _(r):
        row = b * rows + r
        count = counts[row]

        @pl.when(count > per)
        def _():
            for j in range(1, PRE):
                at = pl.ds(r * held + j * per, per)
                merge(r, chunk(
                    r, j * per,
                    kbuf[slot, at].reshape(128, head_dim), vbuf[slot, at].reshape(128, head_dim),
                ))

            @pl.loop(PRE, jnp.maximum((count + per - 1) // per, PRE))
            def _(j):
                @pl.loop(0, jnp.minimum(count - j * per, per))
                def _(s):
                    page = codes[row * max_pages + j * per + s] // code_base
                    first = pltpu.make_async_copy(k_hbm.at[page], kmore.at[s], moresem.at[0])
                    second = pltpu.make_async_copy(v_hbm.at[page], vmore.at[s], moresem.at[1])
                    first.start()
                    second.start()
                    first.wait()
                    second.wait()

                merge(r, chunk(
                    r, j * per, kmore[...].reshape(128, head_dim), vmore[...].reshape(128, head_dim)
                ))


def attend(codes, counts, totals, all_queries, keys, values, page_len, kv_local, code_base, max_pages):
    blocks, rows, q_local, head_dim = all_queries.shape
    span = page_len * kv_local
    per = 128 // span
    held = per * PRE
    unroll = 4
    sizes = (rows, max_pages, span, kv_local, blocks, code_base, unroll)
    return pl.pallas_call(
        functools.partial(attend_kernel, sizes),
        out_shape=(
            jax.ShapeDtypeStruct((blocks, rows, q_local, head_dim), jnp.float32),
            jax.ShapeDtypeStruct((blocks, 2, q_local, 128), jnp.float32),
        ),
        grid_spec=pltpu.PrefetchScalarGridSpec(
            num_scalar_prefetch=3,
            grid=(blocks,),
            in_specs=[
                pl.BlockSpec((None, rows, q_local, head_dim), lambda b, *_: (b, 0, 0, 0)),
                pl.BlockSpec(memory_space=pl.ANY),
                pl.BlockSpec(memory_space=pl.ANY),
            ],
            out_specs=(
                pl.BlockSpec((None, rows, q_local, head_dim), lambda b, *_: (b, 0, 0, 0)),
                pl.BlockSpec((None, 2, q_local, 128), lambda b, *_: (b, 0, 0, 0)),
            ),
            scratch_shapes=[
                pltpu.VMEM((DEPTH, rows * held, span, head_dim), keys.dtype),
                pltpu.VMEM((DEPTH, rows * held, span, head_dim), keys.dtype),
                pltpu.VMEM((per, span, head_dim), keys.dtype),
                pltpu.VMEM((per, span, head_dim), keys.dtype),
                pltpu.SemaphoreType.DMA((DEPTH,)),
                pltpu.SemaphoreType.DMA((DEPTH,)),
                pltpu.SemaphoreType.DMA((2,)),
            ],
        ),
        compiler_params=pltpu.CompilerParams(dimension_semantics=("arbitrary",)),
    )(codes, counts, totals, all_queries, keys, values)


def finish_kernel(
    acc_hbm, stat_hbm, w_hbm, att_out, proj_out,
    got_acc, got_stat, weight, mixed, everyone, part, got_part,
    acc_send, acc_recv, stat_send, stat_recv, own_sem, w_sem,
    att_send, att_recv, part_send, part_recv,
):
    n = lax.axis_size("dp")
    me = lax.axis_index("dp")
    m = lax.axis_size("mp")
    mine = lax.axis_index("mp")
    rows, q_local, head_dim = att_out.shape
    out_rows = proj_out.shape[0]
    pieces = part_send.shape[1]
    width = proj_out.shape[1] // pieces
    load_w = pltpu.make_async_copy(w_hbm, weight, w_sem)
    load_w.start()
    own_acc = pltpu.make_async_copy(acc_hbm.at[me], got_acc.at[0], own_sem.at[0])
    own_stat = pltpu.make_async_copy(stat_hbm.at[me], got_stat.at[0], own_sem.at[1])
    own_acc.start()
    own_stat.start()
    axis_barrier(("dp", "mp"))

    waiting = []
    for step in range(1, n):
        peer = lax.rem(me + step, n)
        for src, dst, send, recv in (
            (stat_hbm, got_stat, stat_send, stat_recv),
            (acc_hbm, got_acc, acc_send, acc_recv),
        ):
            copy = pltpu.make_async_remote_copy(
                src_ref=src.at[peer], dst_ref=dst.at[step],
                send_sem=send.at[step], recv_sem=recv.at[step],
                device_id={"dp": peer}, device_id_type=MESH,
            )
            copy.start()
            waiting.append(copy)
    own_stat.wait()
    own_acc.wait()
    for copy in waiting:
        copy.wait()

    top = got_stat[0, 0]
    for s in range(1, n):
        top = jnp.maximum(top, got_stat[s, 0])
    factors = [jnp.exp(got_stat[s, 0] - top) for s in range(n)]
    mass = factors[0] * got_stat[0, 1]
    for s in range(1, n):
        mass = mass + factors[s] * got_stat[s, 1]
    for r in range(rows):
        total = factors[0][:, r : r + 1] * got_acc[0, r]
        for s in range(1, n):
            total = total + factors[s][:, r : r + 1] * got_acc[s, r]
        result = total / mass[:, r : r + 1]
        mixed[r] = result
        att_out[r] = result.astype(jnp.bfloat16)
    for h in range(q_local):
        everyone[me, :, h * head_dim : (h + 1) * head_dim] = mixed[:, h, :].astype(jnp.bfloat16)

    waiting = []
    for step in range(1, n):
        copy = pltpu.make_async_remote_copy(
            src_ref=everyone.at[me], dst_ref=everyone.at[me],
            send_sem=att_send.at[step], recv_sem=att_recv.at[step],
            device_id={"dp": lax.rem(me + step, n)}, device_id_type=MESH,
        )
        copy.start()
        waiting.append(copy)
    load_w.wait()
    for copy in waiting:
        copy.wait()

    waiting = []
    flat = everyone[...].reshape(n * rows, q_local * head_dim)
    for piece in range(pieces):
        value = jnp.dot(
            flat, weight[:, piece * width : (piece + 1) * width], preferred_element_type=jnp.float32
        )
        part[piece] = value.reshape(m, out_rows, width)
        for step in range(1, m):
            peer = lax.rem(mine + step, m)
            copy = pltpu.make_async_remote_copy(
                src_ref=part.at[piece, peer], dst_ref=got_part.at[piece, step],
                send_sem=part_send.at[step, piece], recv_sem=part_recv.at[step, piece],
                device_id={"mp": peer}, device_id_type=MESH,
            )
            copy.start()
            waiting.append((piece, copy))
    for piece in range(pieces):
        total = part[piece, mine]
        for at, copy in waiting:
            if at == piece:
                copy.wait()
        for step in range(1, m):
            total = total + got_part[piece, step]
        proj_out[:, piece * width : (piece + 1) * width] = total.astype(jnp.bfloat16)


def finish(acc, stat, out_weight):
    n, rows, q_local, head_dim = acc.shape
    m = lax.axis_size("mp")
    depth, columns = out_weight.shape
    out_rows = n * rows // m
    pieces = max(columns // 256, 1)
    width = columns // pieces
    dma = pltpu.SemaphoreType.DMA
    return pl.pallas_call(
        finish_kernel,
        out_shape=(
            jax.ShapeDtypeStruct((rows, q_local, head_dim), jnp.bfloat16),
            jax.ShapeDtypeStruct((out_rows, columns), jnp.bfloat16),
        ),
        in_specs=[pl.BlockSpec(memory_space=pl.ANY)] * 3,
        out_specs=(pl.BlockSpec(memory_space=pltpu.VMEM),) * 2,
        scratch_shapes=[
            pltpu.VMEM((n, rows, q_local, head_dim), jnp.float32),
            pltpu.VMEM((n, 2, q_local, 128), jnp.float32),
            pltpu.VMEM((depth, columns), out_weight.dtype),
            pltpu.VMEM((rows, q_local, head_dim), jnp.float32),
            pltpu.VMEM((n, rows, q_local * head_dim), jnp.bfloat16),
            pltpu.VMEM((pieces, m, out_rows, width), jnp.float32),
            pltpu.VMEM((pieces, m, out_rows, width), jnp.float32),
            dma((n,)), dma((n,)), dma((n,)), dma((n,)), dma((2,)), dma,
            dma((n,)), dma((n,)), dma((m, pieces)), dma((m, pieces)),
        ],
        compiler_params=pltpu.CompilerParams(collective_id=1, has_side_effects=True),
    )(acc, stat, out_weight)


def shards(queries, lookup_sheets, content_sheets, page_table, context_len, out_weight):
    req_rows, max_pages = page_table.shape
    pool_local, page_len, kv_local, head_dim = lookup_sheets.shape
    dp_count = lax.axis_size("dp")
    rows_mine = req_rows // dp_count
    code_base = 2 * page_len
    span = page_len * kv_local
    held = (128 // span) * PRE

    local = page_table - lax.axis_index("dp") * pool_local
    slots = jnp.arange(max_pages, dtype=jnp.int32)
    used = jnp.clip(context_len[:, None] - slots[None, :] * page_len, 0, page_len)
    wanted = (local >= 0) & (local < pool_local) & (used > 0)
    before = (slots[:, None] < slots[None, :]).astype(jnp.bfloat16)
    rank = jnp.dot(
        wanted.astype(jnp.bfloat16), before, preferred_element_type=jnp.float32
    ).astype(jnp.int32)
    code = jnp.where(wanted, local * code_base + used, 0)
    rank = jnp.where(wanted, rank, -1)
    codes = jnp.sum(
        jnp.where(rank[:, None, :] == slots[None, :, None], code[:, None, :], 0), axis=2
    )
    counts = jnp.sum(wanted.astype(jnp.int32), axis=1)
    totals = jnp.sum(jnp.minimum(counts, held).reshape(dp_count, rows_mine), axis=1)

    all_queries = gather_queries(queries)
    acc, stat = attend(
        codes.reshape(-1), counts, totals, all_queries,
        lookup_sheets.reshape(pool_local, span, head_dim),
        content_sheets.reshape(pool_local, span, head_dim),
        page_len, kv_local, code_base, max_pages,
    )
    return finish(acc, stat, out_weight)


def solution(mesh):
    placed = (
        P("dp", "mp", None),
        P("dp", None, "mp", None),
        P("dp", None, "mp", None),
        P(),
        P(),
        P("mp", "dp"),
    )
    return jax.shard_map(
        shards,
        mesh=mesh,
        in_specs=placed,
        out_specs=(P("dp", "mp", None), P("mp", "dp")),
        check_vma=False,
    )
```

```python
import functools

import jax
import jax.numpy as jnp
from jax import lax
from jax.experimental import pallas as pl
from jax.experimental.pallas import tpu as pltpu
from jax.sharding import PartitionSpec as P

MESH = pl.DeviceIdType.MESH
NEG = -1e30
DEPTH = 4
PRE = 2


def axis_barrier(axes):
    barrier = pltpu.get_barrier_semaphore()
    total = 0
    for name in axes:
        n = lax.axis_size(name)
        me = lax.axis_index(name)
        for step in range(1, n):
            pl.semaphore_signal(
                barrier, inc=1, device_id={name: lax.rem(me + step, n)}, device_id_type=MESH
            )
        total += n - 1
    pl.semaphore_wait(barrier, total)


def line_gather(buf, right_sem, left_sem, side_sem, recv_sem):
    n = lax.axis_size("dp")
    me = lax.axis_index("dp")
    length = n // 2
    spot = me // 2
    side = lax.rem(me, 2)

    def send(piece, sem, target):
        return pltpu.make_async_remote_copy(
            src_ref=buf.at[piece], dst_ref=buf.at[piece],
            send_sem=sem, recv_sem=recv_sem.at[piece],
            device_id={"dp": target}, device_id_type=MESH,
        )

    def arrive(piece):
        send(piece, side_sem.at[0], me).wait_recv()

    def to_right(t):
        return send((spot - t) * 2 + side, right_sem.at[t], me + 2)

    def to_left(t):
        return send((spot + t) * 2 + side, left_sem.at[t], me - 2)

    def across(at):
        return send(at * 2 + side, side_sem.at[at], spot * 2 + 1 - side)

    has_right = spot < length - 1
    has_left = spot > 0
    for t in range(length):
        @pl.when(spot - t >= 0)
        def _():
            if t:
                arrive((spot - t) * 2 + side)

            @pl.when(has_right)
            def _():
                to_right(t).start()

            if t:
                across(spot - t).start()

        @pl.when(spot + t < length)
        def _():
            if t:
                arrive((spot + t) * 2 + side)

            @pl.when(has_left)
            def _():
                to_left(t).start()

            across(spot + t).start()

    for at in range(length):
        arrive(at * 2 + 1 - side)
        across(at).wait_send()
    for t in range(length):
        @pl.when((spot - t >= 0) & has_right)
        def _():
            to_right(t).wait_send()

        @pl.when((spot + t < length) & has_left)
        def _():
            to_left(t).wait_send()


def line_sems():
    n = lax.axis_size("dp")
    dma = pltpu.SemaphoreType.DMA
    return [dma((n // 2,)), dma((n // 2,)), dma((n // 2,)), dma((n,))]


def gather_kernel(q_ref, all_ref, own_sem, *sems):
    own = pltpu.make_async_copy(q_ref, all_ref.at[lax.axis_index("dp")], own_sem)
    own.start()
    axis_barrier(("dp",))
    own.wait()
    line_gather(all_ref, *sems)


def gather_queries(queries):
    n = lax.axis_size("dp")
    return pl.pallas_call(
        gather_kernel,
        out_shape=jax.ShapeDtypeStruct((n,) + queries.shape, queries.dtype),
        in_specs=[pl.BlockSpec(memory_space=pltpu.VMEM)],
        out_specs=pl.BlockSpec(memory_space=pltpu.VMEM),
        scratch_shapes=[pltpu.SemaphoreType.DMA] + line_sems(),
        compiler_params=pltpu.CompilerParams(collective_id=0, has_side_effects=True),
    )(queries)


def attend_kernel(
    sizes, codes, counts, totals, q_ref, k_hbm, v_hbm, code_ref, stat_ref,
    acc_ref, kbuf, vbuf, kmore, vmore, ksem, vsem, moresem,
):
    rows, max_pages, span, kv_local, blocks, code_base, unroll = sizes
    q_local, head_dim = q_ref.shape[1:]
    per = 128 // span
    held = per * PRE
    b = pl.program_id(0)
    f32 = jnp.float32

    def issue(block, slot):
        @pl.loop(0, rows)
        def _(r):
            row = block * rows + r

            @pl.loop(0, jnp.minimum(counts[row], held))
            def _(s):
                page = lax.div(codes[row * max_pages + s], code_base)
                pltpu.make_async_copy(k_hbm.at[page], kbuf.at[slot, r * held + s], ksem.at[slot]).start()
                pltpu.make_async_copy(v_hbm.at[page], vbuf.at[slot, r * held + s], vsem.at[slot]).start()

    @pl.when(b == 0)
    def _():
        @pl.loop(0, DEPTH)
        def _(slot):
            @pl.loop(0, rows)
            def _(r):
                vbuf[slot, pl.ds(r * held, held)] = jnp.zeros((held, span, head_dim), vbuf.dtype)

        vmore[...] = jnp.zeros(vmore.shape, vmore.dtype)
        for first in range(min(DEPTH - 1, blocks)):
            issue(first, first)

    @pl.when(b + DEPTH - 1 < blocks)
    def _():
        issue(b + DEPTH - 1, lax.rem(b + DEPTH - 1, DEPTH))

    slot = lax.rem(b, DEPTH)
    total = totals[b]
    for bit in range((rows * held).bit_length()):
        size = 1 << bit
        if size > min(rows * held, k_hbm.shape[0]):
            break

        @pl.when((total >> bit) & 1 == 1)
        def _():
            pltpu.make_async_copy(k_hbm.at[pl.ds(0, size)], kbuf.at[slot, pl.ds(0, size)], ksem.at[slot]).wait()
            pltpu.make_async_copy(v_hbm.at[pl.ds(0, size)], vbuf.at[slot, pl.ds(0, size)], vsem.at[slot]).wait()

    lane = lax.broadcasted_iota(jnp.int32, (per * q_local, 128), 1)
    line = lax.broadcasted_iota(jnp.int32, (per * q_local, 128), 0)
    fits = (lane // span == line // q_local) & (
        lane % kv_local == (line % q_local) // (q_local // kv_local)
    )
    token = jnp.where(fits, (lane % span) // kv_local, code_base)
    stat_lane = lax.broadcasted_iota(jnp.int32, (q_local, 128), 1)
    scale = head_dim ** (-0.5)

    def raw_scores(r, keys):
        return lax.dot_general(
            q_ref[r], keys, (((1,), (1,)), ((), ())), preferred_element_type=f32
        ) * scale

    def chunk(r, first, scores, values):
        row = b * rows + r
        limits = [lax.rem(codes[row * max_pages + first + i], code_base) for i in range(per)]
        limit = jnp.concatenate([jnp.full((q_local, 128), x, jnp.int32) for x in limits], axis=0)
        valid = token < limit
        spread = jnp.where(valid, jnp.concatenate([scores] * per, axis=0), NEG)
        peak = jnp.max(spread, axis=1, keepdims=True)
        weights = jnp.where(valid, jnp.exp(spread - peak), 0.0)
        mass = jnp.sum(weights, axis=1, keepdims=True)
        acc = jnp.dot(weights.astype(jnp.bfloat16), values, preferred_element_type=f32)
        peak = peak.reshape(per, q_local, 1)
        top = jnp.max(peak, axis=0)
        factor = jnp.exp(peak - top[None])
        mass = jnp.sum(mass.reshape(per, q_local, 1) * factor, axis=0)
        acc = jnp.sum(acc.reshape(per, q_local, head_dim) * factor, axis=0)
        return top, mass, acc

    def put_stats(r, stats, top, mass):
        return jnp.where(stat_lane == r, top, stats[0]), jnp.where(stat_lane == r, mass, stats[1])

    def first_chunk(r, stats):
        at = pl.ds(r * held, per)
        top, mass, acc = chunk(
            r, 0, acc_ref[r], vbuf[slot, at].reshape(128, head_dim)
        )
        acc_ref[r] = acc
        return put_stats(r, stats, top, mass)

    def body(i, stats):
        for u in range(unroll):
            stats = first_chunk(i * unroll + u, stats)
        return stats

    @pl.loop(0, rows // unroll)
    def _(i):
        for u in range(unroll):
            r = i * unroll + u
            acc_ref[r] = raw_scores(r, kbuf[slot, pl.ds(r * held, per)].reshape(128, head_dim))

    empty = (jnp.full((q_local, 128), NEG, f32), jnp.zeros((q_local, 128), f32))
    stats = lax.fori_loop(0, rows // unroll, body, empty)
    stat_ref[0], stat_ref[1] = stats

    def merge(r, part):
        top, mass, acc = part
        here = stat_lane == r
        old_top = jnp.max(jnp.where(here, stat_ref[0], NEG), axis=1, keepdims=True)
        old_mass = jnp.sum(jnp.where(here, stat_ref[1], 0.0), axis=1, keepdims=True)
        new_top = jnp.maximum(old_top, top)
        old_f = jnp.exp(old_top - new_top)
        new_f = jnp.exp(top - new_top)
        acc_ref[r] = acc_ref[r] * old_f + acc * new_f
        stat_ref[0] = jnp.where(here, new_top, stat_ref[0])
        stat_ref[1] = jnp.where(here, old_mass * old_f + mass * new_f, stat_ref[1])

    @pl.loop(0, rows)
    def _(r):
        row = b * rows + r
        count = counts[row]

        @pl.when(count > per)
        def _():
            for j in range(1, PRE):
                at = pl.ds(r * held + j * per, per)
                merge(r, chunk(
                    r, j * per,
                    raw_scores(r, kbuf[slot, at].reshape(128, head_dim)),
                    vbuf[slot, at].reshape(128, head_dim),
                ))

            @pl.loop(PRE, jnp.maximum((count + per - 1) // per, PRE))
            def _(j):
                @pl.loop(0, jnp.minimum(count - j * per, per))
                def _(s):
                    page = lax.div(codes[row * max_pages + j * per + s], code_base)
                    first = pltpu.make_async_copy(k_hbm.at[page], kmore.at[s], moresem.at[0])
                    second = pltpu.make_async_copy(v_hbm.at[page], vmore.at[s], moresem.at[1])
                    first.start()
                    second.start()
                    first.wait()
                    second.wait()

                merge(r, chunk(
                    r, j * per, raw_scores(r, kmore[...].reshape(128, head_dim)),
                    vmore[...].reshape(128, head_dim),
                ))

    def encode(i, steps):
        for u in range(unroll):
            r = i * unroll + u
            acc = acc_ref[r]
            step = jnp.max(jnp.abs(acc), axis=1, keepdims=True) * (1.0 / 32767.0)
            inverse = jnp.where(step > 1e-30, 1.0 / jnp.maximum(step, 1e-30), 0.0)
            code_ref[r] = jnp.round(acc * inverse).astype(jnp.int32).astype(jnp.int16)
            steps = jnp.where(stat_lane == r, step, steps)
        return steps

    stat_ref[2] = lax.fori_loop(0, rows // unroll, encode, jnp.zeros((q_local, 128), f32))


def attend(codes, counts, totals, all_queries, keys, values, page_len, kv_local, code_base, max_pages):
    blocks, rows, q_local, head_dim = all_queries.shape
    span = page_len * kv_local
    per = 128 // span
    held = per * PRE
    unroll = 16 if rows % 16 == 0 else 1
    sizes = (rows, max_pages, span, kv_local, blocks, code_base, unroll)
    return pl.pallas_call(
        functools.partial(attend_kernel, sizes),
        out_shape=(
            jax.ShapeDtypeStruct((blocks, rows, q_local, head_dim), jnp.int16),
            jax.ShapeDtypeStruct((blocks, 3, q_local, 128), jnp.float32),
        ),
        grid_spec=pltpu.PrefetchScalarGridSpec(
            num_scalar_prefetch=3,
            grid=(blocks,),
            in_specs=[
                pl.BlockSpec((None, rows, q_local, head_dim), lambda b, *_: (b, 0, 0, 0)),
                pl.BlockSpec(memory_space=pl.ANY),
                pl.BlockSpec(memory_space=pl.ANY),
            ],
            out_specs=(
                pl.BlockSpec((None, rows, q_local, head_dim), lambda b, *_: (b, 0, 0, 0)),
                pl.BlockSpec((None, 3, q_local, 128), lambda b, *_: (b, 0, 0, 0)),
            ),
            scratch_shapes=[
                pltpu.VMEM((rows, q_local, head_dim), jnp.float32),
                pltpu.VMEM((DEPTH, rows * held, span, head_dim), keys.dtype),
                pltpu.VMEM((DEPTH, rows * held, span, head_dim), keys.dtype),
                pltpu.VMEM((per, span, head_dim), keys.dtype),
                pltpu.VMEM((per, span, head_dim), keys.dtype),
                pltpu.SemaphoreType.DMA((DEPTH,)),
                pltpu.SemaphoreType.DMA((DEPTH,)),
                pltpu.SemaphoreType.DMA((2,)),
            ],
        ),
        compiler_params=pltpu.CompilerParams(dimension_semantics=("arbitrary",)),
    )(codes, counts, totals, all_queries, keys, values)


def finish_kernel(
    acc_hbm, stat_hbm, w_hbm, att_out, proj_out,
    got_acc, got_stat, weight, mixed, everyone, part, got_pair, summed, got_part,
    acc_send, acc_recv, stat_send, stat_recv, own_sem, w_sem,
    pair_send, pair_recv, part_send, part_recv,
    right_sem, left_sem, side_sem, line_recv,
):
    n = lax.axis_size("dp")
    me = lax.axis_index("dp")
    m = lax.axis_size("mp")
    mine = lax.axis_index("mp")
    rows, q_local, head_dim = att_out.shape
    out_rows = proj_out.shape[0]
    pieces = pair_send.shape[0]
    width = proj_out.shape[1] // pieces
    load_w = pltpu.make_async_copy(w_hbm, weight, w_sem)
    load_w.start()
    own_acc = pltpu.make_async_copy(acc_hbm.at[me], got_acc.at[0], own_sem.at[0])
    own_stat = pltpu.make_async_copy(stat_hbm.at[me], got_stat.at[0], own_sem.at[1])
    own_acc.start()
    own_stat.start()
    axis_barrier(("dp", "mp"))

    waiting = []
    for step in range(1, n):
        peer = lax.rem(me + step, n)
        for src, dst, send, recv in (
            (stat_hbm, got_stat, stat_send, stat_recv),
            (acc_hbm, got_acc, acc_send, acc_recv),
        ):
            copy = pltpu.make_async_remote_copy(
                src_ref=src.at[peer], dst_ref=dst.at[step],
                send_sem=send.at[step], recv_sem=recv.at[step],
                device_id={"dp": peer}, device_id_type=MESH,
            )
            copy.start()
            waiting.append(copy)
    own_stat.wait()
    own_acc.wait()
    for copy in waiting:
        copy.wait()

    top = got_stat[0, 0]
    for s in range(1, n):
        top = jnp.maximum(top, got_stat[s, 0])
    factors = [jnp.exp(got_stat[s, 0] - top) for s in range(n)]
    mass = factors[0] * got_stat[0, 1]
    for s in range(1, n):
        mass = mass + factors[s] * got_stat[s, 1]
    gains = [factors[s] * got_stat[s, 2] / mass for s in range(n)]
    for r in range(rows):
        result = gains[0][:, r : r + 1] * got_acc[0, r].astype(jnp.float32)
        for s in range(1, n):
            result = result + gains[s][:, r : r + 1] * got_acc[s, r].astype(jnp.float32)
        mixed[r] = result
        att_out[r] = result.astype(jnp.bfloat16)
    for h in range(q_local):
        everyone[me, :, h * head_dim : (h + 1) * head_dim] = mixed[:, h, :].astype(jnp.bfloat16)

    line_gather(everyone, right_sem, left_sem, side_sem, line_recv)
    load_w.wait()

    pair = lax.rem(mine, 2)
    group = mine // 2
    groups = m // 2

    def pair_copy(piece):
        return pltpu.make_async_remote_copy(
            src_ref=part.at[piece, :, 1 - pair], dst_ref=got_pair.at[piece],
            send_sem=pair_send.at[piece], recv_sem=pair_recv.at[piece],
            device_id={"mp": group * 2 + 1 - pair}, device_id_type=MESH,
        )

    def group_copy(piece, step):
        return pltpu.make_async_remote_copy(
            src_ref=summed.at[piece, step], dst_ref=got_part.at[piece, step],
            send_sem=part_send.at[step, piece], recv_sem=part_recv.at[step, piece],
            device_id={"mp": lax.rem(group + step, groups) * 2 + pair}, device_id_type=MESH,
        )

    flat = everyone[...].reshape(n * rows, q_local * head_dim)
    for piece in range(pieces):
        value = jnp.dot(
            flat, weight[:, piece * width : (piece + 1) * width], preferred_element_type=jnp.float32
        )
        part[piece] = value.reshape(groups, 2, out_rows, width)
        pair_copy(piece).start()
    for piece in range(pieces):
        pair_copy(piece).wait()
        for step in range(groups):
            at = lax.rem(group + step, groups)
            summed[piece, step] = part[piece, at, pair] + got_pair[piece, at]
        for step in range(1, groups):
            group_copy(piece, step).start()
    for piece in range(pieces):
        total = summed[piece, 0]
        for step in range(1, groups):
            group_copy(piece, step).wait()
            total = total + got_part[piece, step]
        proj_out[:, piece * width : (piece + 1) * width] = total.astype(jnp.bfloat16)


def finish(acc, stat, out_weight):
    n, rows, q_local, head_dim = acc.shape
    m = lax.axis_size("mp")
    depth, columns = out_weight.shape
    out_rows = n * rows // m
    pieces = max(columns // 256, 1)
    width = columns // pieces
    dma = pltpu.SemaphoreType.DMA
    return pl.pallas_call(
        finish_kernel,
        out_shape=(
            jax.ShapeDtypeStruct((rows, q_local, head_dim), jnp.bfloat16),
            jax.ShapeDtypeStruct((out_rows, columns), jnp.bfloat16),
        ),
        in_specs=[pl.BlockSpec(memory_space=pl.ANY)] * 3,
        out_specs=(pl.BlockSpec(memory_space=pltpu.VMEM),) * 2,
        scratch_shapes=[
            pltpu.VMEM((n, rows, q_local, head_dim), acc.dtype),
            pltpu.VMEM((n, 3, q_local, 128), jnp.float32),
            pltpu.VMEM((depth, columns), out_weight.dtype),
            pltpu.VMEM((rows, q_local, head_dim), jnp.float32),
            pltpu.VMEM((n, rows, q_local * head_dim), jnp.bfloat16),
            pltpu.VMEM((pieces, m // 2, 2, out_rows, width), jnp.float32),
            pltpu.VMEM((pieces, m // 2, out_rows, width), jnp.float32),
            pltpu.VMEM((pieces, m // 2, out_rows, width), jnp.float32),
            pltpu.VMEM((pieces, m // 2, out_rows, width), jnp.float32),
            dma((n,)), dma((n,)), dma((n,)), dma((n,)), dma((2,)), dma,
            dma((pieces,)), dma((pieces,)), dma((m // 2, pieces)), dma((m // 2, pieces)),
        ] + line_sems(),
        compiler_params=pltpu.CompilerParams(collective_id=1, has_side_effects=True),
    )(acc, stat, out_weight)


def shards(queries, lookup_sheets, content_sheets, page_table, context_len, out_weight):
    req_rows, max_pages = page_table.shape
    pool_local, page_len, kv_local, head_dim = lookup_sheets.shape
    dp_count = lax.axis_size("dp")
    rows_mine = req_rows // dp_count
    code_base = 2 * page_len
    span = page_len * kv_local
    held = (128 // span) * PRE

    local = page_table - lax.axis_index("dp") * pool_local
    slots = jnp.arange(max_pages, dtype=jnp.int32)
    used = jnp.clip(context_len[:, None] - slots[None, :] * page_len, 0, page_len)
    wanted = (local >= 0) & (local < pool_local) & (used > 0)
    before = (slots[:, None] < slots[None, :]).astype(jnp.bfloat16)
    rank = jnp.dot(
        wanted.astype(jnp.bfloat16), before, preferred_element_type=jnp.float32
    ).astype(jnp.int32)
    code = jnp.where(wanted, local * code_base + used, 0)
    rank = jnp.where(wanted, rank, -1)
    codes = jnp.sum(
        jnp.where(rank[:, None, :] == slots[None, :, None], code[:, None, :], 0), axis=2
    )
    counts = jnp.sum(wanted.astype(jnp.int32), axis=1)
    totals = jnp.sum(jnp.minimum(counts, held).reshape(dp_count, rows_mine), axis=1)

    all_queries = gather_queries(queries)
    acc, stat = attend(
        codes.reshape(-1), counts, totals, all_queries,
        lookup_sheets.reshape(pool_local, span, head_dim),
        content_sheets.reshape(pool_local, span, head_dim),
        page_len, kv_local, code_base, max_pages,
    )
    return finish(acc, stat, out_weight)


def solution(mesh):
    placed = (
        P("dp", "mp", None),
        P("dp", None, "mp", None),
        P("dp", None, "mp", None),
        P(),
        P(),
        P("mp", "dp"),
    )
    return jax.shard_map(
        shards,
        mesh=mesh,
        in_specs=placed,
        out_specs=(P("dp", "mp", None), P("mp", "dp")),
        check_vma=False,
    )
```

```python
import functools

import jax
import jax.numpy as jnp
from jax import lax
from jax.experimental import pallas as pl
from jax.experimental.pallas import tpu as pltpu
from jax.sharding import PartitionSpec as P

MESH = pl.DeviceIdType.MESH
NEG = -1e30
DEPTH = 4
PRE = 2


def axis_barrier(axes):
    barrier = pltpu.get_barrier_semaphore()
    total = 0
    for name in axes:
        n = lax.axis_size(name)
        me = lax.axis_index(name)
        for step in range(1, n):
            pl.semaphore_signal(
                barrier, inc=1, device_id={name: lax.rem(me + step, n)}, device_id_type=MESH
            )
        total += n - 1
    pl.semaphore_wait(barrier, total)


def line_gather(buf, right_sem, left_sem, side_sem, recv_sem):
    n = lax.axis_size("dp")
    me = lax.axis_index("dp")
    length = n // 2
    spot = me // 2
    side = lax.rem(me, 2)

    def send(piece, sem, target):
        return pltpu.make_async_remote_copy(
            src_ref=buf.at[piece], dst_ref=buf.at[piece],
            send_sem=sem, recv_sem=recv_sem.at[piece],
            device_id={"dp": target}, device_id_type=MESH,
        )

    def arrive(piece):
        send(piece, side_sem.at[0], me).wait_recv()

    def to_right(t):
        return send((spot - t) * 2 + side, right_sem.at[t], me + 2)

    def to_left(t):
        return send((spot + t) * 2 + side, left_sem.at[t], me - 2)

    def across(at):
        return send(at * 2 + side, side_sem.at[at], spot * 2 + 1 - side)

    has_right = spot < length - 1
    has_left = spot > 0
    for t in range(length):
        @pl.when(spot - t >= 0)
        def _():
            if t:
                arrive((spot - t) * 2 + side)

            @pl.when(has_right)
            def _():
                to_right(t).start()

            if t:
                across(spot - t).start()

        @pl.when(spot + t < length)
        def _():
            if t:
                arrive((spot + t) * 2 + side)

            @pl.when(has_left)
            def _():
                to_left(t).start()

            across(spot + t).start()

    for at in range(length):
        arrive(at * 2 + 1 - side)
        across(at).wait_send()
    for t in range(length):
        @pl.when((spot - t >= 0) & has_right)
        def _():
            to_right(t).wait_send()

        @pl.when((spot + t < length) & has_left)
        def _():
            to_left(t).wait_send()


def line_sems():
    n = lax.axis_size("dp")
    dma = pltpu.SemaphoreType.DMA
    return [dma((n // 2,)), dma((n // 2,)), dma((n // 2,)), dma((n,))]


def gather_kernel(q_ref, all_ref, own_sem, *sems):
    own = pltpu.make_async_copy(q_ref, all_ref.at[lax.axis_index("dp")], own_sem)
    own.start()
    axis_barrier(("dp",))
    own.wait()
    line_gather(all_ref, *sems)


def gather_queries(queries):
    n = lax.axis_size("dp")
    return pl.pallas_call(
        gather_kernel,
        out_shape=jax.ShapeDtypeStruct((n,) + queries.shape, queries.dtype),
        in_specs=[pl.BlockSpec(memory_space=pltpu.VMEM)],
        out_specs=pl.BlockSpec(memory_space=pltpu.VMEM),
        scratch_shapes=[pltpu.SemaphoreType.DMA] + line_sems(),
        compiler_params=pltpu.CompilerParams(collective_id=0, has_side_effects=True),
    )(queries)


def attend_kernel(
    sizes, codes, counts, totals, q_ref, k_hbm, v_hbm, code_ref, stat_ref,
    acc_ref, kbuf, vbuf, kmore, vmore, ksem, vsem, moresem,
):
    rows, max_pages, span, kv_local, blocks, code_base, unroll = sizes
    q_local, head_dim = q_ref.shape[1:]
    per = 128 // span
    held = per * PRE
    b = pl.program_id(0)
    f32 = jnp.float32

    def issue(block, slot):
        @pl.loop(0, rows)
        def _(r):
            row = block * rows + r

            @pl.loop(0, jnp.minimum(counts[row], held))
            def _(s):
                page = lax.div(codes[row * max_pages + s], code_base)
                pltpu.make_async_copy(k_hbm.at[page], kbuf.at[slot, r * held + s], ksem.at[slot]).start()
                pltpu.make_async_copy(v_hbm.at[page], vbuf.at[slot, r * held + s], vsem.at[slot]).start()

    @pl.when(b == 0)
    def _():
        @pl.loop(0, DEPTH)
        def _(slot):
            @pl.loop(0, rows)
            def _(r):
                vbuf[slot, pl.ds(r * held, held)] = jnp.zeros((held, span, head_dim), vbuf.dtype)

        vmore[...] = jnp.zeros(vmore.shape, vmore.dtype)
        for first in range(min(DEPTH - 1, blocks)):
            issue(first, first)

    @pl.when(b + DEPTH - 1 < blocks)
    def _():
        issue(b + DEPTH - 1, lax.rem(b + DEPTH - 1, DEPTH))

    slot = lax.rem(b, DEPTH)
    total = totals[b]
    for bit in range((rows * held).bit_length()):
        size = 1 << bit
        if size > min(rows * held, k_hbm.shape[0]):
            break

        @pl.when((total >> bit) & 1 == 1)
        def _():
            pltpu.make_async_copy(k_hbm.at[pl.ds(0, size)], kbuf.at[slot, pl.ds(0, size)], ksem.at[slot]).wait()
            pltpu.make_async_copy(v_hbm.at[pl.ds(0, size)], vbuf.at[slot, pl.ds(0, size)], vsem.at[slot]).wait()

    lane = lax.broadcasted_iota(jnp.int32, (per * q_local, 128), 1)
    line = lax.broadcasted_iota(jnp.int32, (per * q_local, 128), 0)
    fits = (lane // span == line // q_local) & (
        lane % kv_local == (line % q_local) // (q_local // kv_local)
    )
    token = jnp.where(fits, (lane % span) // kv_local, code_base)
    stat_lane = lax.broadcasted_iota(jnp.int32, (q_local, 128), 1)
    scale = head_dim ** (-0.5)

    def raw_scores(r, keys):
        return lax.dot_general(
            q_ref[r], keys, (((1,), (1,)), ((), ())), preferred_element_type=f32
        ) * scale

    def chunk(r, first, scores, values):
        row = b * rows + r
        limits = [lax.rem(codes[row * max_pages + first + i], code_base) for i in range(per)]
        limit = jnp.concatenate([jnp.full((q_local, 128), x, jnp.int32) for x in limits], axis=0)
        valid = token < limit
        spread = jnp.where(valid, jnp.concatenate([scores] * per, axis=0), NEG)
        peak = jnp.max(spread, axis=1, keepdims=True)
        weights = jnp.where(valid, jnp.exp(spread - peak), 0.0)
        mass = jnp.sum(weights, axis=1, keepdims=True)
        acc = jnp.dot(weights.astype(jnp.bfloat16), values, preferred_element_type=f32)
        peak = peak.reshape(per, q_local, 1)
        top = jnp.max(peak, axis=0)
        factor = jnp.exp(peak - top[None])
        mass = jnp.sum(mass.reshape(per, q_local, 1) * factor, axis=0)
        acc = jnp.sum(acc.reshape(per, q_local, head_dim) * factor, axis=0)
        return top, mass, acc

    def put_stats(r, stats, top, mass):
        return jnp.where(stat_lane == r, top, stats[0]), jnp.where(stat_lane == r, mass, stats[1])

    def first_chunk(r, stats):
        at = pl.ds(r * held, per)
        top, mass, acc = chunk(
            r, 0, acc_ref[r], vbuf[slot, at].reshape(128, head_dim)
        )
        acc_ref[r] = acc
        return put_stats(r, stats, top, mass)

    def body(i, stats):
        for u in range(unroll):
            stats = first_chunk(i * unroll + u, stats)
        return stats

    @pl.loop(0, rows // unroll)
    def _(i):
        for u in range(unroll):
            r = i * unroll + u
            acc_ref[r] = raw_scores(r, kbuf[slot, pl.ds(r * held, per)].reshape(128, head_dim))

    empty = (jnp.full((q_local, 128), NEG, f32), jnp.zeros((q_local, 128), f32))
    stats = lax.fori_loop(0, rows // unroll, body, empty)
    stat_ref[0], stat_ref[1] = stats

    def merge(r, part):
        top, mass, acc = part
        here = stat_lane == r
        old_top = jnp.max(jnp.where(here, stat_ref[0], NEG), axis=1, keepdims=True)
        old_mass = jnp.sum(jnp.where(here, stat_ref[1], 0.0), axis=1, keepdims=True)
        new_top = jnp.maximum(old_top, top)
        old_f = jnp.exp(old_top - new_top)
        new_f = jnp.exp(top - new_top)
        acc_ref[r] = acc_ref[r] * old_f + acc * new_f
        stat_ref[0] = jnp.where(here, new_top, stat_ref[0])
        stat_ref[1] = jnp.where(here, old_mass * old_f + mass * new_f, stat_ref[1])

    @pl.loop(0, rows)
    def _(r):
        row = b * rows + r
        count = counts[row]

        @pl.when(count > per)
        def _():
            for j in range(1, PRE):
                at = pl.ds(r * held + j * per, per)
                merge(r, chunk(
                    r, j * per,
                    raw_scores(r, kbuf[slot, at].reshape(128, head_dim)),
                    vbuf[slot, at].reshape(128, head_dim),
                ))

            @pl.loop(PRE, jnp.maximum((count + per - 1) // per, PRE))
            def _(j):
                @pl.loop(0, jnp.minimum(count - j * per, per))
                def _(s):
                    page = lax.div(codes[row * max_pages + j * per + s], code_base)
                    first = pltpu.make_async_copy(k_hbm.at[page], kmore.at[s], moresem.at[0])
                    second = pltpu.make_async_copy(v_hbm.at[page], vmore.at[s], moresem.at[1])
                    first.start()
                    second.start()
                    first.wait()
                    second.wait()

                merge(r, chunk(
                    r, j * per, raw_scores(r, kmore[...].reshape(128, head_dim)),
                    vmore[...].reshape(128, head_dim),
                ))

    def encode(i, steps):
        for u in range(unroll):
            r = i * unroll + u
            acc = acc_ref[r]
            step = jnp.max(jnp.abs(acc), axis=1, keepdims=True) * (1.0 / 32767.0)
            floor = jnp.maximum(step, 1e-30)
            inverse = 1.0 / floor
            inverse = jnp.where(step > 1e-30, inverse * (2.0 - floor * inverse), 0.0)
            code_ref[r] = jnp.round(acc * inverse).astype(jnp.int32).astype(jnp.int16)
            steps = jnp.where(stat_lane == r, step, steps)
        return steps

    stat_ref[2] = lax.fori_loop(0, rows // unroll, encode, jnp.zeros((q_local, 128), f32))


def attend(codes, counts, totals, all_queries, keys, values, page_len, kv_local, code_base, max_pages):
    blocks, rows, q_local, head_dim = all_queries.shape
    span = page_len * kv_local
    per = 128 // span
    held = per * PRE
    unroll = 32 if rows % 32 == 0 else 1
    sizes = (rows, max_pages, span, kv_local, blocks, code_base, unroll)
    return pl.pallas_call(
        functools.partial(attend_kernel, sizes),
        out_shape=(
            jax.ShapeDtypeStruct((blocks, rows, q_local, head_dim), jnp.int16),
            jax.ShapeDtypeStruct((blocks, 3, q_local, 128), jnp.float32),
        ),
        grid_spec=pltpu.PrefetchScalarGridSpec(
            num_scalar_prefetch=3,
            grid=(blocks,),
            in_specs=[
                pl.BlockSpec((None, rows, q_local, head_dim), lambda b, *_: (b, 0, 0, 0)),
                pl.BlockSpec(memory_space=pl.ANY),
                pl.BlockSpec(memory_space=pl.ANY),
            ],
            out_specs=(
                pl.BlockSpec((None, rows, q_local, head_dim), lambda b, *_: (b, 0, 0, 0)),
                pl.BlockSpec((None, 3, q_local, 128), lambda b, *_: (b, 0, 0, 0)),
            ),
            scratch_shapes=[
                pltpu.VMEM((rows, q_local, head_dim), jnp.float32),
                pltpu.VMEM((DEPTH, rows * held, span, head_dim), keys.dtype),
                pltpu.VMEM((DEPTH, rows * held, span, head_dim), keys.dtype),
                pltpu.VMEM((per, span, head_dim), keys.dtype),
                pltpu.VMEM((per, span, head_dim), keys.dtype),
                pltpu.SemaphoreType.DMA((DEPTH,)),
                pltpu.SemaphoreType.DMA((DEPTH,)),
                pltpu.SemaphoreType.DMA((2,)),
            ],
        ),
        compiler_params=pltpu.CompilerParams(dimension_semantics=("arbitrary",)),
    )(codes, counts, totals, all_queries, keys, values)


def finish_kernel(
    acc_hbm, stat_hbm, w_hbm, att_out, proj_out,
    got_acc, got_stat, weight, mixed, everyone, part, got_pair, summed, got_part,
    acc_send, acc_recv, stat_send, stat_recv, own_sem, w_sem,
    pair_send, pair_recv, part_send, part_recv,
    right_sem, left_sem, side_sem, line_recv,
):
    n = lax.axis_size("dp")
    me = lax.axis_index("dp")
    m = lax.axis_size("mp")
    mine = lax.axis_index("mp")
    rows, q_local, head_dim = att_out.shape
    out_rows = proj_out.shape[0]
    pieces = pair_send.shape[0]
    width = proj_out.shape[1] // pieces
    load_w = pltpu.make_async_copy(w_hbm, weight, w_sem)
    load_w.start()
    own_acc = pltpu.make_async_copy(acc_hbm.at[me], got_acc.at[0], own_sem.at[0])
    own_stat = pltpu.make_async_copy(stat_hbm.at[me], got_stat.at[0], own_sem.at[1])
    own_acc.start()
    own_stat.start()
    axis_barrier(("dp", "mp"))

    stat_copies, acc_copies = [None], [None]
    for step in range(1, n):
        peer = lax.rem(me + step, n)
        for src, dst, send, recv, copies in (
            (stat_hbm, got_stat, stat_send, stat_recv, stat_copies),
            (acc_hbm, got_acc, acc_send, acc_recv, acc_copies),
        ):
            copies.append(pltpu.make_async_remote_copy(
                src_ref=src.at[peer], dst_ref=dst.at[step],
                send_sem=send.at[step], recv_sem=recv.at[step],
                device_id={"dp": peer}, device_id_type=MESH,
            ))
    for copies in (stat_copies, acc_copies):
        for copy in copies[1:]:
            copy.start()
    own_stat.wait()
    for copy in stat_copies[1:]:
        copy.wait()

    top = got_stat[0, 0]
    for s in range(1, n):
        top = jnp.maximum(top, got_stat[s, 0])
    factors = [jnp.exp(got_stat[s, 0] - top) for s in range(n)]
    mass = factors[0] * got_stat[0, 1]
    for s in range(1, n):
        mass = mass + factors[s] * got_stat[s, 1]
    gains = [factors[s] * got_stat[s, 2] / mass for s in range(n)]
    own_acc.wait()
    for s in range(n):
        if s:
            acc_copies[s].wait()
        for r in range(rows):
            term = gains[s][:, r : r + 1] * got_acc[s, r].astype(jnp.float32)
            mixed[r] = mixed[r] + term if s else term
    att_out[...] = mixed[...].astype(jnp.bfloat16)
    for h in range(q_local):
        everyone[me, :, h * head_dim : (h + 1) * head_dim] = mixed[:, h, :].astype(jnp.bfloat16)

    line_gather(everyone, right_sem, left_sem, side_sem, line_recv)
    load_w.wait()

    pair = lax.rem(mine, 2)
    group = mine // 2
    groups = m // 2

    def pair_copy(piece):
        return pltpu.make_async_remote_copy(
            src_ref=part.at[piece, :, 1 - pair], dst_ref=got_pair.at[piece],
            send_sem=pair_send.at[piece], recv_sem=pair_recv.at[piece],
            device_id={"mp": group * 2 + 1 - pair}, device_id_type=MESH,
        )

    def group_copy(piece, step):
        return pltpu.make_async_remote_copy(
            src_ref=summed.at[piece, step], dst_ref=got_part.at[piece, step],
            send_sem=part_send.at[step, piece], recv_sem=part_recv.at[step, piece],
            device_id={"mp": lax.rem(group + step, groups) * 2 + pair}, device_id_type=MESH,
        )

    flat = everyone[...].reshape(n * rows, q_local * head_dim)
    for piece in range(pieces):
        value = jnp.dot(
            flat, weight[:, piece * width : (piece + 1) * width], preferred_element_type=jnp.float32
        )
        part[piece] = value.reshape(groups, 2, out_rows, width)
        pair_copy(piece).start()
    for piece in range(pieces):
        pair_copy(piece).wait()
        for step in range(groups):
            at = lax.rem(group + step, groups)
            summed[piece, step] = part[piece, at, pair] + got_pair[piece, at]
        for step in range(1, groups):
            group_copy(piece, step).start()
    for piece in range(pieces):
        total = summed[piece, 0]
        for step in range(1, groups):
            group_copy(piece, step).wait()
            total = total + got_part[piece, step]
        proj_out[:, piece * width : (piece + 1) * width] = total.astype(jnp.bfloat16)


def finish(acc, stat, out_weight):
    n, rows, q_local, head_dim = acc.shape
    m = lax.axis_size("mp")
    depth, columns = out_weight.shape
    out_rows = n * rows // m
    pieces = max(columns // 256, 1)
    width = columns // pieces
    dma = pltpu.SemaphoreType.DMA
    return pl.pallas_call(
        finish_kernel,
        out_shape=(
            jax.ShapeDtypeStruct((rows, q_local, head_dim), jnp.bfloat16),
            jax.ShapeDtypeStruct((out_rows, columns), jnp.bfloat16),
        ),
        in_specs=[pl.BlockSpec(memory_space=pl.ANY)] * 3,
        out_specs=(pl.BlockSpec(memory_space=pltpu.VMEM),) * 2,
        scratch_shapes=[
            pltpu.VMEM((n, rows, q_local, head_dim), acc.dtype),
            pltpu.VMEM((n, 3, q_local, 128), jnp.float32),
            pltpu.VMEM((depth, columns), out_weight.dtype),
            pltpu.VMEM((rows, q_local, head_dim), jnp.float32),
            pltpu.VMEM((n, rows, q_local * head_dim), jnp.bfloat16),
            pltpu.VMEM((pieces, m // 2, 2, out_rows, width), jnp.float32),
            pltpu.VMEM((pieces, m // 2, out_rows, width), jnp.float32),
            pltpu.VMEM((pieces, m // 2, out_rows, width), jnp.float32),
            pltpu.VMEM((pieces, m // 2, out_rows, width), jnp.float32),
            dma((n,)), dma((n,)), dma((n,)), dma((n,)), dma((2,)), dma,
            dma((pieces,)), dma((pieces,)), dma((m // 2, pieces)), dma((m // 2, pieces)),
        ] + line_sems(),
        compiler_params=pltpu.CompilerParams(collective_id=1, has_side_effects=True),
    )(acc, stat, out_weight)


def shards(queries, lookup_sheets, content_sheets, page_table, context_len, out_weight):
    req_rows, max_pages = page_table.shape
    pool_local, page_len, kv_local, head_dim = lookup_sheets.shape
    dp_count = lax.axis_size("dp")
    rows_mine = req_rows // dp_count
    code_base = 2 * page_len
    span = page_len * kv_local
    held = (128 // span) * PRE

    local = page_table - lax.axis_index("dp") * pool_local
    slots = jnp.arange(max_pages, dtype=jnp.int32)
    used = jnp.clip(context_len[:, None] - slots[None, :] * page_len, 0, page_len)
    wanted = (local >= 0) & (local < pool_local) & (used > 0)
    before = (slots[:, None] < slots[None, :]).astype(jnp.bfloat16)
    rank = jnp.dot(
        wanted.astype(jnp.bfloat16), before, preferred_element_type=jnp.float32
    ).astype(jnp.int32)
    code = jnp.where(wanted, local * code_base + used, 0)
    rank = jnp.where(wanted, rank, -1)
    codes = jnp.sum(
        jnp.where(rank[:, None, :] == slots[None, :, None], code[:, None, :], 0), axis=2
    )
    counts = jnp.sum(wanted.astype(jnp.int32), axis=1)
    totals = jnp.sum(jnp.minimum(counts, held).reshape(dp_count, rows_mine), axis=1)

    all_queries = gather_queries(queries)
    acc, stat = attend(
        codes.reshape(-1), counts, totals, all_queries,
        lookup_sheets.reshape(pool_local, span, head_dim),
        content_sheets.reshape(pool_local, span, head_dim),
        page_len, kv_local, code_base, max_pages,
    )
    return finish(acc, stat, out_weight)


def solution(mesh):
    placed = (
        P("dp", "mp", None),
        P("dp", None, "mp", None),
        P("dp", None, "mp", None),
        P(),
        P(),
        P("mp", "dp"),
    )
    return jax.shard_map(
        shards,
        mesh=mesh,
        in_specs=placed,
        out_specs=(P("dp", "mp", None), P("mp", "dp")),
        check_vma=False,
    )
```

```python
import functools

import jax
import jax.numpy as jnp
from jax import lax
from jax.experimental import pallas as pl
from jax.experimental.pallas import tpu as pltpu
from jax.sharding import PartitionSpec as P

MESH = pl.DeviceIdType.MESH
NEG = -1e30
DEPTH = 4
PRE = 2
PARTS = 2


def axis_barrier(axes):
    barrier = pltpu.get_barrier_semaphore()
    total = 0
    for name in axes:
        n = lax.axis_size(name)
        me = lax.axis_index(name)
        for step in range(1, n):
            pl.semaphore_signal(
                barrier, inc=1, device_id={name: lax.rem(me + step, n)}, device_id_type=MESH
            )
        total += n - 1
    pl.semaphore_wait(barrier, total)


def line_gather(buf, right_sem, left_sem, side_sem, recv_sem):
    n = lax.axis_size("dp")
    me = lax.axis_index("dp")
    length = n // 2
    spot = me // 2
    side = lax.rem(me, 2)

    half = buf.shape[1] // PARTS

    def send(piece, h, sem, target):
        at = buf.at[piece, pl.ds(h * half, half)]
        return pltpu.make_async_remote_copy(
            src_ref=at, dst_ref=at, send_sem=sem, recv_sem=recv_sem.at[piece, h],
            device_id={"dp": target}, device_id_type=MESH,
        )

    def arrive(piece, h):
        send(piece, h, side_sem.at[0, h], me).wait_recv()

    def to_right(t, h):
        return send((spot - t) * 2 + side, h, right_sem.at[t, h], me + 2)

    def to_left(t, h):
        return send((spot + t) * 2 + side, h, left_sem.at[t, h], me - 2)

    def across(at, h):
        return send(at * 2 + side, h, side_sem.at[at, h], spot * 2 + 1 - side)

    has_right = spot < length - 1
    has_left = spot > 0
    for t in range(length):
        for h in range(PARTS):
            @pl.when(spot - t >= 0)
            def _():
                if t:
                    arrive((spot - t) * 2 + side, h)

                @pl.when(has_right)
                def _():
                    to_right(t, h).start()

                if t:
                    across(spot - t, h).start()

            @pl.when(spot + t < length)
            def _():
                if t:
                    arrive((spot + t) * 2 + side, h)

                @pl.when(has_left)
                def _():
                    to_left(t, h).start()

                across(spot + t, h).start()

    for h in range(PARTS):
        for at in range(length):
            arrive(at * 2 + 1 - side, h)
            across(at, h).wait_send()
        for t in range(length):
            @pl.when((spot - t >= 0) & has_right)
            def _():
                to_right(t, h).wait_send()

            @pl.when((spot + t < length) & has_left)
            def _():
                to_left(t, h).wait_send()


def line_sems():
    n = lax.axis_size("dp")
    dma = pltpu.SemaphoreType.DMA
    return [dma((n // 2, PARTS)), dma((n // 2, PARTS)), dma((n // 2, PARTS)), dma((n, PARTS))]


def gather_kernel(q_ref, all_ref, own_sem, *sems):
    own = pltpu.make_async_copy(q_ref, all_ref.at[lax.axis_index("dp")], own_sem)
    own.start()
    axis_barrier(("dp",))
    own.wait()
    line_gather(all_ref, *sems)


def gather_queries(queries):
    n = lax.axis_size("dp")
    return pl.pallas_call(
        gather_kernel,
        out_shape=jax.ShapeDtypeStruct((n,) + queries.shape, queries.dtype),
        in_specs=[pl.BlockSpec(memory_space=pltpu.VMEM)],
        out_specs=pl.BlockSpec(memory_space=pltpu.VMEM),
        scratch_shapes=[pltpu.SemaphoreType.DMA] + line_sems(),
        compiler_params=pltpu.CompilerParams(collective_id=0, has_side_effects=True),
    )(queries)


def attend_kernel(
    sizes, codes, counts, totals, q_ref, k_hbm, v_hbm, code_ref, stat_ref,
    acc_ref, kbuf, vbuf, kmore, vmore, ksem, vsem, moresem,
):
    rows, max_pages, span, kv_local, blocks, code_base, unroll = sizes
    q_local, head_dim = q_ref.shape[1:]
    per = 128 // span
    held = per * PRE
    b = pl.program_id(0)
    f32 = jnp.float32

    def issue(block, slot):
        @pl.loop(0, rows)
        def _(r):
            row = block * rows + r

            @pl.loop(0, jnp.minimum(counts[row], held))
            def _(s):
                page = lax.div(codes[row * max_pages + s], code_base)
                pltpu.make_async_copy(k_hbm.at[page], kbuf.at[slot, r * held + s], ksem.at[slot]).start()
                pltpu.make_async_copy(v_hbm.at[page], vbuf.at[slot, r * held + s], vsem.at[slot]).start()

    @pl.when(b == 0)
    def _():
        @pl.loop(0, DEPTH)
        def _(slot):
            @pl.loop(0, rows)
            def _(r):
                vbuf[slot, pl.ds(r * held, held)] = jnp.zeros((held, span, head_dim), vbuf.dtype)

        vmore[...] = jnp.zeros(vmore.shape, vmore.dtype)
        for first in range(min(DEPTH - 1, blocks)):
            issue(first, first)

    @pl.when(b + DEPTH - 1 < blocks)
    def _():
        issue(b + DEPTH - 1, lax.rem(b + DEPTH - 1, DEPTH))

    slot = lax.rem(b, DEPTH)
    total = totals[b]
    for bit in range((rows * held).bit_length()):
        size = 1 << bit
        if size > min(rows * held, k_hbm.shape[0]):
            break

        @pl.when((total >> bit) & 1 == 1)
        def _():
            pltpu.make_async_copy(k_hbm.at[pl.ds(0, size)], kbuf.at[slot, pl.ds(0, size)], ksem.at[slot]).wait()
            pltpu.make_async_copy(v_hbm.at[pl.ds(0, size)], vbuf.at[slot, pl.ds(0, size)], vsem.at[slot]).wait()

    lane = lax.broadcasted_iota(jnp.int32, (per * q_local, 128), 1)
    line = lax.broadcasted_iota(jnp.int32, (per * q_local, 128), 0)
    fits = (lane // span == line // q_local) & (
        lane % kv_local == (line % q_local) // (q_local // kv_local)
    )
    token = jnp.where(fits, (lane % span) // kv_local, code_base)
    stat_lane = lax.broadcasted_iota(jnp.int32, (q_local, 128), 1)
    scale = head_dim ** (-0.5)

    def raw_scores(r, keys):
        return lax.dot_general(
            q_ref[r], keys, (((1,), (1,)), ((), ())), preferred_element_type=f32
        ) * scale

    def chunk(r, first, scores, values):
        row = b * rows + r
        limits = [lax.rem(codes[row * max_pages + first + i], code_base) for i in range(per)]
        limit = jnp.concatenate([jnp.full((q_local, 128), x, jnp.int32) for x in limits], axis=0)
        valid = token < limit
        spread = jnp.where(valid, jnp.concatenate([scores] * per, axis=0), NEG)
        peak = jnp.max(spread, axis=1, keepdims=True)
        weights = jnp.where(valid, jnp.exp(spread - peak), 0.0)
        mass = jnp.sum(weights, axis=1, keepdims=True)
        acc = jnp.dot(weights.astype(jnp.bfloat16), values, preferred_element_type=f32)
        peak = peak.reshape(per, q_local, 1)
        top = jnp.max(peak, axis=0)
        factor = jnp.exp(peak - top[None])
        mass = jnp.sum(mass.reshape(per, q_local, 1) * factor, axis=0)
        acc = jnp.sum(acc.reshape(per, q_local, head_dim) * factor, axis=0)
        return top, mass, acc

    def put_stats(r, stats, top, mass):
        return jnp.where(stat_lane == r, top, stats[0]), jnp.where(stat_lane == r, mass, stats[1])

    def first_chunk(r, stats):
        at = pl.ds(r * held, per)
        top, mass, acc = chunk(
            r, 0, acc_ref[r], vbuf[slot, at].reshape(128, head_dim)
        )
        acc_ref[r] = acc
        return put_stats(r, stats, top, mass)

    def body(i, stats):
        for u in range(unroll):
            stats = first_chunk(i * unroll + u, stats)
        return stats

    @pl.loop(0, rows // unroll)
    def _(i):
        for u in range(unroll):
            r = i * unroll + u
            acc_ref[r] = raw_scores(r, kbuf[slot, pl.ds(r * held, per)].reshape(128, head_dim))

    empty = (jnp.full((q_local, 128), NEG, f32), jnp.zeros((q_local, 128), f32))
    stats = lax.fori_loop(0, rows // unroll, body, empty)
    stat_ref[0], stat_ref[1] = stats

    def merge(r, part):
        top, mass, acc = part
        here = stat_lane == r
        old_top = jnp.max(jnp.where(here, stat_ref[0], NEG), axis=1, keepdims=True)
        old_mass = jnp.sum(jnp.where(here, stat_ref[1], 0.0), axis=1, keepdims=True)
        new_top = jnp.maximum(old_top, top)
        old_f = jnp.exp(old_top - new_top)
        new_f = jnp.exp(top - new_top)
        acc_ref[r] = acc_ref[r] * old_f + acc * new_f
        stat_ref[0] = jnp.where(here, new_top, stat_ref[0])
        stat_ref[1] = jnp.where(here, old_mass * old_f + mass * new_f, stat_ref[1])

    @pl.loop(0, rows)
    def _(r):
        row = b * rows + r
        count = counts[row]

        @pl.when(count > per)
        def _():
            for j in range(1, PRE):
                at = pl.ds(r * held + j * per, per)
                merge(r, chunk(
                    r, j * per,
                    raw_scores(r, kbuf[slot, at].reshape(128, head_dim)),
                    vbuf[slot, at].reshape(128, head_dim),
                ))

            @pl.loop(PRE, jnp.maximum((count + per - 1) // per, PRE))
            def _(j):
                @pl.loop(0, jnp.minimum(count - j * per, per))
                def _(s):
                    page = lax.div(codes[row * max_pages + j * per + s], code_base)
                    first = pltpu.make_async_copy(k_hbm.at[page], kmore.at[s], moresem.at[0])
                    second = pltpu.make_async_copy(v_hbm.at[page], vmore.at[s], moresem.at[1])
                    first.start()
                    second.start()
                    first.wait()
                    second.wait()

                merge(r, chunk(
                    r, j * per, raw_scores(r, kmore[...].reshape(128, head_dim)),
                    vmore[...].reshape(128, head_dim),
                ))

    def encode(i, steps):
        for u in range(unroll):
            r = i * unroll + u
            acc = acc_ref[r]
            step = jnp.max(jnp.abs(acc), axis=1, keepdims=True) * (1.0 / 32767.0)
            floor = jnp.maximum(step, 1e-30)
            inverse = 1.0 / floor
            inverse = jnp.where(step > 1e-30, inverse * (2.0 - floor * inverse), 0.0)
            code_ref[r] = jnp.round(acc * inverse).astype(jnp.int32).astype(jnp.int16)
            steps = jnp.where(stat_lane == r, step, steps)
        return steps

    stat_ref[2] = lax.fori_loop(0, rows // unroll, encode, jnp.zeros((q_local, 128), f32))


def attend(codes, counts, totals, all_queries, keys, values, page_len, kv_local, code_base, max_pages):
    blocks, rows, q_local, head_dim = all_queries.shape
    span = page_len * kv_local
    per = 128 // span
    held = per * PRE
    unroll = 32 if rows % 32 == 0 else 1
    sizes = (rows, max_pages, span, kv_local, blocks, code_base, unroll)
    return pl.pallas_call(
        functools.partial(attend_kernel, sizes),
        out_shape=(
            jax.ShapeDtypeStruct((blocks, rows, q_local, head_dim), jnp.int16),
            jax.ShapeDtypeStruct((blocks, 3, q_local, 128), jnp.float32),
        ),
        grid_spec=pltpu.PrefetchScalarGridSpec(
            num_scalar_prefetch=3,
            grid=(blocks,),
            in_specs=[
                pl.BlockSpec((None, rows, q_local, head_dim), lambda b, *_: (b, 0, 0, 0)),
                pl.BlockSpec(memory_space=pl.ANY),
                pl.BlockSpec(memory_space=pl.ANY),
            ],
            out_specs=(
                pl.BlockSpec((None, rows, q_local, head_dim), lambda b, *_: (b, 0, 0, 0)),
                pl.BlockSpec((None, 3, q_local, 128), lambda b, *_: (b, 0, 0, 0)),
            ),
            scratch_shapes=[
                pltpu.VMEM((rows, q_local, head_dim), jnp.float32),
                pltpu.VMEM((DEPTH, rows * held, span, head_dim), keys.dtype),
                pltpu.VMEM((DEPTH, rows * held, span, head_dim), keys.dtype),
                pltpu.VMEM((per, span, head_dim), keys.dtype),
                pltpu.VMEM((per, span, head_dim), keys.dtype),
                pltpu.SemaphoreType.DMA((DEPTH,)),
                pltpu.SemaphoreType.DMA((DEPTH,)),
                pltpu.SemaphoreType.DMA((2,)),
            ],
        ),
        compiler_params=pltpu.CompilerParams(dimension_semantics=("arbitrary",)),
    )(codes, counts, totals, all_queries, keys, values)


def finish_kernel(
    acc_hbm, stat_hbm, w_hbm, att_out, proj_out,
    got_acc, got_stat, weight, mixed, everyone, part, got_pair, summed, got_part,
    acc_send, acc_recv, stat_send, stat_recv, own_sem, w_sem,
    pair_send, pair_recv, part_send, part_recv,
    right_sem, left_sem, side_sem, line_recv,
):
    n = lax.axis_size("dp")
    me = lax.axis_index("dp")
    m = lax.axis_size("mp")
    mine = lax.axis_index("mp")
    rows, q_local, head_dim = att_out.shape
    out_rows = proj_out.shape[0]
    pieces = pair_send.shape[0]
    width = proj_out.shape[1] // pieces
    load_w = pltpu.make_async_copy(w_hbm, weight, w_sem)
    load_w.start()
    own_acc = pltpu.make_async_copy(acc_hbm.at[me], got_acc.at[0], own_sem.at[0])
    own_stat = pltpu.make_async_copy(stat_hbm.at[me], got_stat.at[0], own_sem.at[1])
    own_acc.start()
    own_stat.start()
    axis_barrier(("dp", "mp"))

    stat_copies, acc_copies = [None], [None]
    for step in range(1, n):
        peer = lax.rem(me + step, n)
        for src, dst, send, recv, copies in (
            (stat_hbm, got_stat, stat_send, stat_recv, stat_copies),
            (acc_hbm, got_acc, acc_send, acc_recv, acc_copies),
        ):
            copies.append(pltpu.make_async_remote_copy(
                src_ref=src.at[peer], dst_ref=dst.at[step],
                send_sem=send.at[step], recv_sem=recv.at[step],
                device_id={"dp": peer}, device_id_type=MESH,
            ))
    for copies in (stat_copies, acc_copies):
        for copy in copies[1:]:
            copy.start()
    own_stat.wait()
    for copy in stat_copies[1:]:
        copy.wait()

    top = got_stat[0, 0]
    for s in range(1, n):
        top = jnp.maximum(top, got_stat[s, 0])
    factors = [jnp.exp(got_stat[s, 0] - top) for s in range(n)]
    mass = factors[0] * got_stat[0, 1]
    for s in range(1, n):
        mass = mass + factors[s] * got_stat[s, 1]
    gains = [factors[s] * got_stat[s, 2] / mass for s in range(n)]
    own_acc.wait()
    for s in range(n):
        if s:
            acc_copies[s].wait()
        for r in range(rows):
            term = gains[s][:, r : r + 1] * got_acc[s, r].astype(jnp.float32)
            mixed[r] = mixed[r] + term if s else term
    att_out[...] = mixed[...].astype(jnp.bfloat16)
    for h in range(q_local):
        everyone[me, :, h * head_dim : (h + 1) * head_dim] = mixed[:, h, :].astype(jnp.bfloat16)

    line_gather(everyone, right_sem, left_sem, side_sem, line_recv)
    load_w.wait()

    pair = lax.rem(mine, 2)
    group = mine // 2
    groups = m // 2

    def pair_copy(piece):
        return pltpu.make_async_remote_copy(
            src_ref=part.at[piece, :, 1 - pair], dst_ref=got_pair.at[piece],
            send_sem=pair_send.at[piece], recv_sem=pair_recv.at[piece],
            device_id={"mp": group * 2 + 1 - pair}, device_id_type=MESH,
        )

    def group_copy(piece, step):
        return pltpu.make_async_remote_copy(
            src_ref=summed.at[piece, step], dst_ref=got_part.at[piece, step],
            send_sem=part_send.at[step, piece], recv_sem=part_recv.at[step, piece],
            device_id={"mp": lax.rem(group + step, groups) * 2 + pair}, device_id_type=MESH,
        )

    flat = everyone[...].reshape(n * rows, q_local * head_dim)
    for piece in range(pieces):
        value = jnp.dot(
            flat, weight[:, piece * width : (piece + 1) * width], preferred_element_type=jnp.float32
        )
        part[piece] = value.reshape(groups, 2, out_rows, width)
        pair_copy(piece).start()
    for piece in range(pieces):
        pair_copy(piece).wait()
        for step in range(groups):
            at = lax.rem(group + step, groups)
            summed[piece, step] = part[piece, at, pair] + got_pair[piece, at]
        for step in range(1, groups):
            group_copy(piece, step).start()
    for piece in range(pieces):
        total = summed[piece, 0]
        for step in range(1, groups):
            group_copy(piece, step).wait()
            total = total + got_part[piece, step]
        proj_out[:, piece * width : (piece + 1) * width] = total.astype(jnp.bfloat16)


def finish(acc, stat, out_weight):
    n, rows, q_local, head_dim = acc.shape
    m = lax.axis_size("mp")
    depth, columns = out_weight.shape
    out_rows = n * rows // m
    pieces = max(columns // 256, 1)
    width = columns // pieces
    dma = pltpu.SemaphoreType.DMA
    return pl.pallas_call(
        finish_kernel,
        out_shape=(
            jax.ShapeDtypeStruct((rows, q_local, head_dim), jnp.bfloat16),
            jax.ShapeDtypeStruct((out_rows, columns), jnp.bfloat16),
        ),
        in_specs=[pl.BlockSpec(memory_space=pl.ANY)] * 3,
        out_specs=(pl.BlockSpec(memory_space=pltpu.VMEM),) * 2,
        scratch_shapes=[
            pltpu.VMEM((n, rows, q_local, head_dim), acc.dtype),
            pltpu.VMEM((n, 3, q_local, 128), jnp.float32),
            pltpu.VMEM((depth, columns), out_weight.dtype),
            pltpu.VMEM((rows, q_local, head_dim), jnp.float32),
            pltpu.VMEM((n, rows, q_local * head_dim), jnp.bfloat16),
            pltpu.VMEM((pieces, m // 2, 2, out_rows, width), jnp.float32),
            pltpu.VMEM((pieces, m // 2, out_rows, width), jnp.float32),
            pltpu.VMEM((pieces, m // 2, out_rows, width), jnp.float32),
            pltpu.VMEM((pieces, m // 2, out_rows, width), jnp.float32),
            dma((n,)), dma((n,)), dma((n,)), dma((n,)), dma((2,)), dma,
            dma((pieces,)), dma((pieces,)), dma((m // 2, pieces)), dma((m // 2, pieces)),
        ] + line_sems(),
        compiler_params=pltpu.CompilerParams(collective_id=1, has_side_effects=True),
    )(acc, stat, out_weight)


def shards(queries, lookup_sheets, content_sheets, page_table, context_len, out_weight):
    req_rows, max_pages = page_table.shape
    pool_local, page_len, kv_local, head_dim = lookup_sheets.shape
    dp_count = lax.axis_size("dp")
    rows_mine = req_rows // dp_count
    code_base = 2 * page_len
    span = page_len * kv_local
    held = (128 // span) * PRE

    local = page_table - lax.axis_index("dp") * pool_local
    slots = jnp.arange(max_pages, dtype=jnp.int32)
    used = jnp.clip(context_len[:, None] - slots[None, :] * page_len, 0, page_len)
    wanted = (local >= 0) & (local < pool_local) & (used > 0)
    before = (slots[:, None] < slots[None, :]).astype(jnp.bfloat16)
    rank = jnp.dot(
        wanted.astype(jnp.bfloat16), before, preferred_element_type=jnp.float32
    ).astype(jnp.int32)
    code = jnp.where(wanted, local * code_base + used, 0)
    rank = jnp.where(wanted, rank, -1)
    codes = jnp.sum(
        jnp.where(rank[:, None, :] == slots[None, :, None], code[:, None, :], 0), axis=2
    )
    counts = jnp.sum(wanted.astype(jnp.int32), axis=1)
    totals = jnp.sum(jnp.minimum(counts, held).reshape(dp_count, rows_mine), axis=1)

    all_queries = gather_queries(queries)
    acc, stat = attend(
        codes.reshape(-1), counts, totals, all_queries,
        lookup_sheets.reshape(pool_local, span, head_dim),
        content_sheets.reshape(pool_local, span, head_dim),
        page_len, kv_local, code_base, max_pages,
    )
    return finish(acc, stat, out_weight)


def solution(mesh):
    placed = (
        P("dp", "mp", None),
        P("dp", None, "mp", None),
        P("dp", None, "mp", None),
        P(),
        P(),
        P("mp", "dp"),
    )
    return jax.shard_map(
        shards,
        mesh=mesh,
        in_specs=placed,
        out_specs=(P("dp", "mp", None), P("mp", "dp")),
        check_vma=False,
    )
```
